32 devices in a mesh: seq: 8 (over y, x, core), batch: 4 (over z).
Axes of the slice: x: 2, y: 2, z: 4, core: 2. Of those that a mesh axis runs over, the one named last changes fastest.
Arguments:
- queries: bfloat16 [4, 4096, 256], P('batch', 'seq'), may hold values from -6 to 6
- key_rows: bfloat16 [4, 4096, 256], P('batch', 'seq'), may hold values from -6 to 6
- value_rows: bfloat16 [4, 4096, 256], P('batch', 'seq'), may hold values from -6 to 6
- step_rates: float32 [4, 4096], P('batch', 'seq'), may hold values from 0.02 to 0.2
- cotangent: bfloat16 [4, 4096, 256], P('batch', 'seq'), may hold values from -0.046875 to 0.046875
- fast_init: float32 [768, 256], P('batch'), may hold values from -0.375 to 0.375
Outputs:
- layer_out: bfloat16 [4, 4096, 256], P('batch', 'seq')
- init_grad: float32 [768, 256], P('batch')
The draws below stay inside these ranges and needn't reach their ends.
All inputs are finite; a program needn't handle non-finite values.
Results may differ from the reference program's by a relative error of at most 0.0012.
Values sent between devices are 32-bit elements; how exact they have to be, the bound alone decides.
No kernel may reach another device: no remote copies, remote signals or barrier semaphores. Data moves between devices by JAX's collectives and lax.ppermute only.
A program may use at most 64 MiB of HBM per device.

```python
import math
import jax
import jax.numpy as jnp
from jax import lax

HD = 256
FH = 256
SEQ_LEN = 4096
SEQS = 4


def level_of(rng, shape, pieces, smallest, largest):
    level = 1.0
    for axis_at, shards_of in pieces:
        steps = jax.random.uniform(jax.random.fold_in(jax.random.fold_in(rng, 6), axis_at), (shards_of,), jnp.float32, smallest / len(pieces), largest / len(pieces))
        level = level * jnp.repeat(jnp.exp(steps), shape[axis_at] // shards_of).reshape((-1,) + (1,) * (len(shape) - 1 - axis_at))
    return level


def gaussian(key, dims, spread, bound, split=(), held_as=jnp.bfloat16):
    drawn = spread * jax.random.normal(key, dims, jnp.float32)
    if split:
        drawn = drawn * level_of(key, dims, split, -0.22, 0.18)
    return jnp.clip(drawn, -bound, bound).astype(held_as)


def setup_inputs(seed: int = 0) -> dict:
    streams_of = jax.random.split(jax.random.key(seed), 7)
    queries = gaussian(streams_of[0], (SEQS, SEQ_LEN, HD), 1.0, 6.0, ((0, 4), (1, 8)))
    key_rows = gaussian(streams_of[1], (SEQS, SEQ_LEN, HD), 1.0, 6.0, ((0, 4), (1, 8)))
    value_rows = gaussian(streams_of[2], (SEQS, SEQ_LEN, HD), 1.0, 6.0, ((0, 4), (1, 8)))
    step_rates = jnp.clip(jnp.exp(math.log(0.2) - 2.3025851 * jax.random.uniform(streams_of[3], (SEQS, SEQ_LEN), jnp.float32) ** level_of(streams_of[3], (SEQS, SEQ_LEN), ((0, 4), (1, 8)), -0.2, 0.2)), 0.02, 0.2)
    cotangent = gaussian(streams_of[4], (SEQS, SEQ_LEN, HD), ((SEQ_LEN * SEQS) ** -0.5), 0.046875, ((0, 4), (1, 8)))
    fast_init = gaussian(streams_of[5], (3 * HD, FH), HD ** -0.5, 0.375, ((0, 4),), jnp.float32)
    return dict(queries=queries, key_rows=key_rows, value_rows=value_rows, step_rates=step_rates, cotangent=cotangent, fast_init=fast_init)


def swiglu_apply(weights, row_block):
    high = lax.Precision.HIGHEST
    projected = jnp.dot(row_block, weights[0], precision=high, preferred_element_type=jnp.float32)
    gate_pre = jnp.dot(row_block, weights[1], precision=high, preferred_element_type=jnp.float32)
    hidden = jax.nn.silu(gate_pre) * projected
    return jnp.dot(hidden, weights[2].T, precision=high, preferred_element_type=jnp.float32)

def inner_loss(weights, key_block, value_block, scaled):
    return -jnp.sum(scaled[:, None] * swiglu_apply(weights, key_block) * value_block)

def inner_grad(weights, key_block, value_block, scaled):
    return jax.grad(inner_loss)(weights, key_block, value_block, scaled)

def reference(queries, key_rows, value_rows, step_rates, cotangent, fast_init):
    initial = fast_init.reshape(3, HD, FH)
    divisor = math.sqrt(SEQ_LEN)

    def one_sequence(items):
        query_seq, key_seq, value_seq, rate_seq, cot_seq = items
        query_block = query_seq.astype(jnp.float32)
        key_block = key_seq.astype(jnp.float32)
        value_block = value_seq.astype(jnp.float32)
        scaled = rate_seq / divisor

        def forward(weights):
            middle = weights - inner_grad(weights, key_block, value_block, scaled)
            final = middle - inner_grad(middle, key_block, value_block, scaled)
            return swiglu_apply(final, query_block)
        result, pull_back = jax.vjp(forward, initial)
        grads = pull_back(cot_seq.astype(jnp.float32))[0]
        return (result.astype(jnp.bfloat16), grads)
    outputs, grads = lax.map(one_sequence, (queries, key_rows, value_rows, step_rates, cotangent))
    return (outputs, lax.optimization_barrier(jnp.sum(grads, axis=0)).reshape(3 * HD, FH))
```

```python
import math

import jax
import jax.numpy as jnp
from jax import lax
from jax.experimental import pallas as pl
from jax.experimental.pallas import tpu as pltpu
from jax.sharding import PartitionSpec as P

F32 = jnp.float32
BF16 = jnp.bfloat16
PAD = 8
PAIRED = 8


def nt(left, right):
    return lax.dot_general(left, right, (((1,), (1,)), ((), ())), preferred_element_type=F32)


def nn(left, right):
    return lax.dot_general(left, right, (((1,), (0,)), ((), ())), preferred_element_type=F32)


def tn(left, right):
    return lax.dot_general(left, right, (((0,), (0,)), ((), ())), preferred_element_type=F32)


def two_terms(x):
    high = x.astype(BF16).astype(F32)
    return jnp.concatenate([x, x - high], axis=0).astype(BF16)


def fold(x):
    half = x.shape[0] // 2
    return x[:half] + x[half:]


def gate(g):
    decay = jnp.exp(-jnp.abs(g))
    sig = jnp.where(g >= 0, 1.0, decay) / (1.0 + decay)
    silu = g * sig
    slope = sig + silu * (1.0 - sig)
    return sig, silu, slope


def ascent_terms(stack_ab, stack_c, units, keys, values, eta):
    pre = fold(nt(stack_ab, keys))
    p, g = pre[:units], pre[units:]
    e = eta * fold(nt(stack_c, values))
    _, silu, slope = gate(g)
    pair = jnp.concatenate([e * silu, e * p * slope], axis=0)
    hidden = eta * (silu * p)
    return fold(nn(two_terms(pair), keys)), fold(nn(two_terms(hidden), values))


def curvature_terms(stack_ab, stack_c, units, keys, values, eta):
    pre = fold(nt(stack_ab, keys))
    p, g = pre[:units], pre[units : 2 * units]
    tp, tg = pre[2 * units : 3 * units], pre[3 * units :]
    both = fold(nt(stack_c, values))
    e, te = eta * both[:units], eta * both[units:]
    sig, silu, slope = gate(g)
    bend = sig * (1.0 - sig) * (2.0 + g * (1.0 - 2.0 * sig))
    slope_tg = slope * tg
    pair = jnp.concatenate(
        [te * silu + e * slope_tg, slope * (te * p + e * tp) + e * p * (bend * tg)], axis=0
    )
    hidden = eta * (slope_tg * p + silu * tp)
    return fold(nn(two_terms(pair), keys)), fold(nn(two_terms(hidden), values))


def flat(ref):
    return jnp.concatenate([ref[0], ref[1]], axis=0), ref[2]


def split_message(ref, tokens, width):
    return (
        ref[:tokens, :width].astype(BF16),
        ref[:tokens, width:].astype(BF16),
        ref[tokens : tokens + PAD, :tokens],
    )


def sweep(terms, stack_ab, stack_c, units, width, stores, acc):
    for kv, eta in stores:
        count, _, tokens = eta.shape

        def step(i, acc, kv=kv, eta=eta, tokens=tokens):
            start = i * tokens if isinstance(i, int) else pl.multiple_of(i * tokens, tokens)
            rows = pl.ds(start, tokens)
            ab, c = terms(
                stack_ab, stack_c, units, kv[rows, :width], kv[rows, width:], eta[i, 0:1, :]
            )
            return acc[0] + ab, acc[1] + c

        if count <= PAIRED:
            for i in range(count):
                acc = step(i, acc)
        else:
            acc = lax.fori_loop(0, count, step, acc)
    return acc


def first_kernel(messages, columns, units, width, *refs):
    if columns:
        place_ref, pieces, refs = refs[0], refs[1 : 1 + columns], refs[1 + columns :]
        parts, (base_ref, acc_ref, kv_ref, eta_ref, blocks) = refs[:messages], refs[messages:]
        mine = place_ref[0]
        for k, piece in enumerate(pieces):
            blocks[lax.rem(mine - k + columns, columns)] = piece[...]
        rows = jnp.concatenate([blocks[k] for k in range(columns)], axis=1)
        for j in range(3):
            base_ref[j] = rows[:, j * width : (j + 1) * width]
        start_ref = base_ref
    else:
        start_ref, base_ref = refs[0], refs[1]
        parts, (acc_ref, kv_ref, eta_ref) = refs[2 : 2 + messages], refs[2 + messages :]
    tokens = parts[0].shape[0] - PAD
    ab, c = flat(base_ref)
    stack_ab, stack_c = two_terms(ab), two_terms(c)
    acc = flat(start_ref)
    for i, part in enumerate(parts):
        keys, values, eta = split_message(part, tokens, width)
        kv_ref[i * tokens : (i + 1) * tokens, :width] = keys
        kv_ref[i * tokens : (i + 1) * tokens, width:] = values
        eta_ref[i] = eta
        more = ascent_terms(stack_ab, stack_c, units, keys, values, eta[0:1, :])
        acc = acc[0] + more[0], acc[1] + more[1]
    acc_ref[0], acc_ref[1], acc_ref[2] = acc[0][:units], acc[0][units:], acc[1]


def second_kernel(stored, units, width, *refs):
    start_ref = refs[0]
    stores = [(refs[1 + 2 * i], refs[2 + 2 * i]) for i in range(stored)]
    out_ref = refs[1 + 2 * stored]
    ab, c = flat(start_ref)
    ab, c = sweep(ascent_terms, two_terms(ab), two_terms(c), units, width, stores, (ab, c))
    out_ref[0], out_ref[1], out_ref[2] = ab[:units], ab[units:], c


def outer_kernel(groups, stacked, units, width, *refs):
    weights = [refs[0].at[j] for j in range(groups)] if stacked else refs[:groups]
    refs = refs[1:] if stacked else refs[groups:]
    queries, cots = refs[0], refs[1]
    tokens = queries.shape[0]
    twin = len(refs) > 2 and refs[2].shape == (tokens, 2 * width) and refs[2].dtype == F32
    other = refs[2] if twin else None
    refs = refs[3:] if twin else refs[2:]
    outs = refs[:2] if twin else refs[:1]
    refs = refs[len(outs) :]
    grads = [refs[0].at[j] for j in range(groups)] if stacked else refs
    hidden_units = groups * units
    ab = jnp.concatenate([w[0] for w in weights] + [w[1] for w in weights], axis=0)
    c = jnp.concatenate([w[2] for w in weights], axis=0)
    stack_ab, stack_c = two_terms(ab), two_terms(c)
    c_high = stack_c[:hidden_units]
    c_three = jnp.concatenate([c_high, c_high, stack_c[hidden_units:]], axis=0)
    total = None
    for index, out_ref in enumerate(outs):
        if index == 0:
            q, cot = queries[...], cots[...]
        else:
            q, cot = other[:, :width].astype(BF16), other[:, width:].astype(BF16)
        pre = fold(nt(stack_ab, q))
        p, g = pre[:hidden_units], pre[hidden_units:]
        e = fold(nt(stack_c, cot))
        _, silu, slope = gate(g)
        hidden = silu * p
        pair = jnp.concatenate([e * silu, e * p * slope], axis=0)
        d_ab = fold(nn(two_terms(pair), q))
        hidden_two = two_terms(hidden)
        d_c = fold(nn(hidden_two, cot))
        lifted = jnp.concatenate([hidden_two, hidden_two[:hidden_units]], axis=0)
        out_ref[...] = tn(lifted, c_three).astype(out_ref.dtype)
        total = (d_ab, d_c) if total is None else (total[0] + d_ab, total[1] + d_c)
    for j, grad in enumerate(grads):
        grad[0] = total[0][j * units : (j + 1) * units]
        grad[1] = total[0][hidden_units + j * units : hidden_units + (j + 1) * units]
        grad[2] = total[1][j * units : (j + 1) * units]


def adjoint_kernel(stored, terms, units, width, parts, *refs):
    place_ref, first_ref, second_ref = refs[:3]
    adjoints = refs[3 : 3 + terms]
    stores = [(refs[3 + terms + 2 * i], refs[4 + terms + 2 * i]) for i in range(stored)]
    refs = refs[3 + terms + 2 * stored :]
    outs, (held, bases, blocks) = refs[:parts], refs[parts:]
    u_ab, u_c = flat(adjoints[0])
    for more in adjoints[1:]:
        ab, c = flat(more)
        u_ab, u_c = u_ab + ab, u_c + c
    held[0], held[1], held[2] = u_ab[:units], u_ab[units:], u_c
    bases[0], bases[1] = second_ref[...], first_ref[...]

    def step(i, carry):
        u_ab, u_c = flat(held)
        ab, c = flat(bases.at[i])
        stack_ab = two_terms(jnp.concatenate([ab, u_ab], axis=0))
        stack_c = two_terms(jnp.concatenate([c, u_c], axis=0))
        u_ab, u_c = sweep(curvature_terms, stack_ab, stack_c, units, width, stores, (u_ab, u_c))
        held[0], held[1], held[2] = u_ab[:units], u_ab[units:], u_c
        return carry

    lax.fori_loop(0, 2, step, 0)
    u_ab, u_c = flat(held)
    rows = jnp.concatenate([u_ab[:units], u_ab[units:], u_c], axis=1)
    share = rows.shape[1] // parts
    mine = place_ref[0]
    for target in range(parts):
        blocks[target] = rows[:, target * share : (target + 1) * share]
    for k, out_ref in enumerate(outs):
        out_ref[...] = blocks[lax.rem(mine + k, parts)]


def final_kernel(paired, units, *refs):
    place_ref = refs[0]
    parts = refs[1:-2]
    out_ref, held = refs[-2:]
    if paired:
        here = place_ref[0]
        for mask, part in enumerate(parts):
            source = here ^ mask
            place = (source & 1) * (PAIRED // 2) + (source >> 1)
            held[pl.ds(pl.multiple_of(place * units, units), units), :] = part[...]
    else:
        for j in range(parts[0].shape[0]):
            held[j * units : (j + 1) * units, :] = parts[0][j]
    out_ref[...] = held[...].T


def prepare_kernel(paired, *refs):
    place_ref, keys, values, rates, weights, first, second, column, held = refs
    half, width = keys.shape[0] // 2, keys.shape[1]
    units = column.shape[0]
    for at, message in ((0, first), (half, second)):
        message[:half, :width] = keys[at : at + half, :].astype(F32)
        message[:half, width:] = values[at : at + half, :].astype(F32)
        message[half:, :half] = jnp.broadcast_to(rates[:, at : at + half], (PAD, half))
        message[half:, half:] = jnp.zeros((PAD, 2 * width - half), F32)
    held[...] = weights[...].T
    here = place_ref[0]
    group = (here & 1) * (PAIRED // 2) + (here >> 1) if paired else here
    column[...] = held[pl.ds(pl.multiple_of(group * units, units), units), :]


def size_of(x):
    return math.prod(x.shape) * x.dtype.itemsize


def call(kernel, out_shape, cost, inputs, smem=(), scratch=()):
    specs = [
        pl.BlockSpec(memory_space=pltpu.SMEM if i in smem else pltpu.VMEM)
        for i in range(len(inputs))
    ]
    out_specs = jax.tree.map(lambda _: pl.BlockSpec(memory_space=pltpu.VMEM), out_shape)
    held = sum(size_of(x) for x in list(inputs) + jax.tree.leaves(out_shape))
    return pl.pallas_call(
        kernel,
        out_shape=out_shape,
        in_specs=specs,
        out_specs=out_specs,
        scratch_shapes=list(scratch),
        compiler_params=pltpu.CompilerParams(
            vmem_limit_bytes=min(60 * 1024 * 1024, held + 12 * 1024 * 1024)
        ),
        cost_estimate=pl.CostEstimate(flops=cost, bytes_accessed=0, transcendentals=0),
    )(*inputs)


def body(queries, key_rows, value_rows, step_rates, cotangent, fast_init):
    tokens, width = queries.shape[1:]
    hidden = fast_init.shape[1]
    shards = lax.axis_size("seq")
    parts = lax.axis_size("batch")
    units = hidden // shards
    divisor = math.sqrt(shards * tokens)
    here = lax.axis_index("seq").astype(jnp.int32)[None]
    row = lax.axis_index("batch").astype(jnp.int32)[None]
    paired = shards == PAIRED
    half = tokens // 2
    share = 3 * width // parts
    block = jax.ShapeDtypeStruct((3, units, width), F32)
    column_block = jax.ShapeDtypeStruct((units, share), F32)

    def swap(x, mask):
        return lax.ppermute(x, "seq", [(i, i ^ mask) for i in range(shards)])

    def turn(x, k):
        return lax.ppermute(x, "batch", [(i, (i + k) % parts) for i in range(parts)])

    packed = jax.ShapeDtypeStruct((half + PAD, 2 * width), F32)
    *own, column = call(
        lambda *refs: prepare_kernel(paired, *refs),
        (packed, packed, column_block),
        1000,
        [here, key_rows[0], value_rows[0], step_rates / divisor, fast_init],
        smem=(0,),
        scratch=[pltpu.VMEM((hidden, share), F32)],
    )

    def first(start, messages):
        count = len(messages)
        outs = (
            block,
            jax.ShapeDtypeStruct((count * half, 2 * width), BF16),
            jax.ShapeDtypeStruct((count, PAD, half), F32),
        )
        columns = 0 if len(start) == 2 else len(start) - 1
        return call(
            lambda *refs: first_kernel(count, columns, units, width, *refs),
            (block,) * (columns > 0) + outs,
            2 * 2 * 6 * count * half * width * units,
            start + messages,
            smem=(0,) if columns else (),
            scratch=[pltpu.VMEM((parts, units, share), F32)] if columns else (),
        )

    if paired:
        x = [None, None]
        y = [None, None]
        x[0], y[1] = swap(own[0], 2), swap(own[1], 4)
        columns = [column] + [turn(column, k) for k in range(1, parts)]
        x[1], y[0] = swap(own[1], 2), swap(own[0], 4)
        diagonal = [swap(x[0], 4), swap(y[1], 2)]
        near = own + [swap(m, 1) for m in own]
        side = x + y
        side = side + [swap(m, 1) for m in side]
        far = diagonal + [swap(m, 1) for m in diagonal]
        initial, partial, *store_a = first([row] + columns, near)
        partial, *store_b = first([partial, initial], side)
        middle, *store_c = first([partial, initial], far)
        stores = [*store_a, *store_b, *store_c]
    else:
        initial = lax.all_gather(column, "batch", axis=1, tiled=True)
        initial = jnp.stack(jnp.split(initial, 3, axis=1))
        every = lax.all_gather(jnp.stack(own), "seq", axis=0, tiled=True)
        kv = every[:, :half].astype(BF16).reshape(2 * shards * half, 2 * width)
        stores = [kv, every[:, half:, :half]]
        middle = None

    def ascend(base):
        return call(
            lambda *refs: second_kernel(len(stores) // 2, units, width, *refs),
            block,
            2 * 2 * 6 * shards * tokens * width * units,
            [base] + stores,
        )

    if middle is None:
        middle = ascend(initial)
    last = ascend(middle)

    cost = 2 * 2 * 7 * tokens * width * hidden
    if paired:
        pair = jnp.concatenate([queries[0].astype(F32), cotangent[0].astype(F32)], axis=1)
        other = swap(pair, 1)
        weights = [last, swap(last, 2), swap(last, 4), swap(last, 6)]
        part = jax.ShapeDtypeStruct((tokens, width), F32)
        kept, given, *grads = call(
            lambda *refs: outer_kernel(4, False, units, width, *refs),
            (part, part) + (block,) * 4,
            cost,
            weights + [queries[0], cotangent[0], other],
        )
        adjoints = [grads[0], swap(grads[1], 2), swap(grads[2], 4), swap(grads[3], 6)]
        result = (kept + swap(given, 1)).astype(BF16)
        result, adjoints[0] = lax.optimization_barrier((result, adjoints[0]))
    else:
        weights = lax.all_gather(last, "seq", axis=0, tiled=False)
        result, grads = call(
            lambda *refs: outer_kernel(shards, True, units, width, *refs),
            (
                jax.ShapeDtypeStruct((tokens, width), BF16),
                jax.ShapeDtypeStruct((shards, 3, units, width), F32),
            ),
            cost,
            [weights, queries[0], cotangent[0]],
        )
        adjoints = [lax.psum_scatter(grads, "seq", scatter_dimension=0, tiled=False)]

    rolled = call(
        lambda *refs: adjoint_kernel(len(stores) // 2, len(adjoints), units, width, parts, *refs),
        (column_block,) * parts,
        2 * 2 * 24 * shards * tokens * width * units,
        [row, initial, middle] + adjoints + stores,
        smem=(0,),
        scratch=[
            pltpu.VMEM((3, units, width), F32),
            pltpu.VMEM((2, 3, units, width), F32),
            pltpu.VMEM((parts, units, share), F32),
        ],
    )
    summed = rolled[0]
    for k in range(1, parts):
        summed = summed + turn(rolled[k], k)
    if paired:
        ring = [summed] + [swap(summed, mask) for mask in (2, 4, 6)]
        pieces = []
        for piece in ring:
            pieces += [piece, swap(piece, 1)]
    else:
        pieces = [lax.all_gather(summed, "seq", axis=0, tiled=False)]
    grad = call(
        lambda *refs: final_kernel(paired, units, *refs),
        jax.ShapeDtypeStruct((share, hidden), F32),
        1000,
        [here] + pieces,
        smem=(0,),
        scratch=[pltpu.VMEM((hidden, share), F32)],
    )
    return result[None], grad


def solution(mesh):
    placed = (
        P("batch", "seq", None),
        P("batch", "seq", None),
        P("batch", "seq", None),
        P("batch", "seq"),
        P("batch", "seq", None),
        P("batch", None),
    )
    return jax.shard_map(
        body,
        mesh=mesh,
        in_specs=placed,
        out_specs=(P("batch", "seq", None), P("batch", None)),
        check_vma=False,
    )
```

```python
import math

import jax
import jax.numpy as jnp
from jax import lax
from jax.experimental import pallas as pl
from jax.experimental.pallas import tpu as pltpu
from jax.sharding import PartitionSpec as P


F32 = jnp.float32
BF16 = jnp.bfloat16
PAD = 8
PAIRED = 8
CHUNK = 1024
MIB = 1024 * 1024


def nt(left, right):
    return lax.dot_general(left, right, (((1,), (1,)), ((), ())), preferred_element_type=F32)


def nn(left, right):
    return lax.dot_general(left, right, (((1,), (0,)), ((), ())), preferred_element_type=F32)


def tn(left, right):
    return lax.dot_general(left, right, (((0,), (0,)), ((), ())), preferred_element_type=F32)


def two_terms(x):
    high = x.astype(BF16).astype(F32)
    return jnp.concatenate([x, x - high], axis=0).astype(BF16)


def fold(x):
    half = x.shape[0] // 2
    return x[:half] + x[half:]


def gate(g):
    decay = jnp.exp(-jnp.abs(g))
    sig = jnp.where(g >= 0, 1.0, decay) / (1.0 + decay)
    silu = g * sig
    slope = sig + silu * (1.0 - sig)
    return sig, silu, slope


def forward(stack_ab, stack_c, keys, values):
    return nt(stack_ab, keys), nt(stack_c, values)


def ascent_terms(units, pre, cross, keys, values, eta):
    pre = fold(pre)
    p, g = pre[:units], pre[units:]
    e = eta * fold(cross)
    _, silu, slope = gate(g)
    pair = jnp.concatenate([e * silu, e * p * slope], axis=0)
    hidden = eta * (silu * p)
    return fold(nn(two_terms(pair), keys)), fold(nn(two_terms(hidden), values))


def curvature_terms(units, pre, cross, keys, values, eta):
    pre = fold(pre)
    p, g = pre[:units], pre[units : 2 * units]
    tp, tg = pre[2 * units : 3 * units], pre[3 * units :]
    both = fold(cross)
    e, te = eta * both[:units], eta * both[units:]
    sig, silu, slope = gate(g)
    bend = sig * (1.0 - sig) * (2.0 + g * (1.0 - 2.0 * sig))
    slope_tg = slope * tg
    pair = jnp.concatenate(
        [te * silu + e * slope_tg, slope * (te * p + e * tp) + e * p * (bend * tg)], axis=0
    )
    hidden = eta * (slope_tg * p + silu * tp)
    return fold(nn(two_terms(pair), keys)), fold(nn(two_terms(hidden), values))


def flat(ref):
    return jnp.concatenate([ref[0], ref[1]], axis=0), ref[2]


def sweep(terms, stack_ab, stack_c, units, stores, acc):
    def load(kv, eta, start, size):
        width = kv.shape[1] // 2
        rows = pl.ds(start, size)
        return kv[rows, :width], kv[rows, width:], eta[0:1, rows]

    chunks = [
        (kv, eta, start, min(CHUNK, kv.shape[0] - start))
        for kv, eta in stores
        for start in range(0, kv.shape[0], CHUNK)
    ]
    if len(chunks) <= PAIRED:
        now = load(*chunks[0])
        pre = forward(stack_ab, stack_c, *now[:2])
        for i in range(len(chunks)):
            if i + 1 < len(chunks):
                later = load(*chunks[i + 1])
                ahead = forward(stack_ab, stack_c, *later[:2])
            ab, c = terms(units, *pre, *now)
            acc = acc[0] + ab, acc[1] + c
            if i + 1 < len(chunks):
                now, pre = later, ahead
        return acc
    for kv, eta in stores:

        def step(i, acc, kv=kv, eta=eta):
            now = load(kv, eta, pl.multiple_of(i * CHUNK, CHUNK), CHUNK)
            ab, c = terms(units, *forward(stack_ab, stack_c, *now[:2]), *now)
            return acc[0] + ab, acc[1] + c

        acc = lax.fori_loop(0, kv.shape[0] // CHUNK, step, acc)
    return acc


def first_kernel(messages, columns, units, width, *refs):
    if columns:
        place_ref, pieces, refs = refs[0], refs[1 : 1 + columns], refs[1 + columns :]
        parts, (base_ref, acc_ref, kv_ref, eta_ref, blocks) = refs[:messages], refs[messages:]
        mine = place_ref[0]
        for k, piece in enumerate(pieces):
            blocks[lax.rem(mine - k + columns, columns)] = piece[...]
        rows = jnp.concatenate([blocks[k] for k in range(columns)], axis=1)
        for j in range(3):
            base_ref[j] = rows[:, j * width : (j + 1) * width]
        start_ref = base_ref
    else:
        start_ref, base_ref = refs[0], refs[1]
        parts, (acc_ref, kv_ref, eta_ref) = refs[2 : 2 + messages], refs[2 + messages :]
    tokens = parts[0].shape[0] - PAD
    for i, part in enumerate(parts):
        rows = pl.ds(i * tokens, tokens)
        kv_ref[rows, :] = part[:tokens, :].astype(BF16)
        eta_ref[:, rows] = part[tokens:, :tokens]
    ab, c = flat(base_ref)
    acc = sweep(
        ascent_terms, two_terms(ab), two_terms(c), units, [(kv_ref, eta_ref)], flat(start_ref)
    )
    acc_ref[0], acc_ref[1], acc_ref[2] = acc[0][:units], acc[0][units:], acc[1]


def second_kernel(stored, units, *refs):
    start_ref = refs[0]
    stores = [(refs[1 + 2 * i], refs[2 + 2 * i]) for i in range(stored)]
    out_ref = refs[1 + 2 * stored]
    ab, c = flat(start_ref)
    ab, c = sweep(ascent_terms, two_terms(ab), two_terms(c), units, stores, (ab, c))
    out_ref[0], out_ref[1], out_ref[2] = ab[:units], ab[units:], c


def outer_kernel(groups, stacked, units, width, *refs):
    weights = [refs[0].at[j] for j in range(groups)] if stacked else refs[:groups]
    refs = refs[1:] if stacked else refs[groups:]
    queries, cots = refs[0], refs[1]
    tokens = queries.shape[0]
    twin = len(refs) > 2 and refs[2].shape == (tokens, 2 * width) and refs[2].dtype == F32
    other = refs[2] if twin else None
    refs = refs[3:] if twin else refs[2:]
    outs = refs[:2] if twin else refs[:1]
    refs = refs[len(outs) :]
    grads = [refs[0].at[j] for j in range(groups)] if stacked else refs
    hidden_units = groups * units
    ab = jnp.concatenate([w[0] for w in weights] + [w[1] for w in weights], axis=0)
    c = jnp.concatenate([w[2] for w in weights], axis=0)
    stack_ab, stack_c = two_terms(ab), two_terms(c)
    c_high = stack_c[:hidden_units]
    c_three = jnp.concatenate([c_high, c_high, stack_c[hidden_units:]], axis=0)
    total = None
    for index, out_ref in enumerate(outs):
        if index == 0:
            q, cot = queries[...], cots[...]
        else:
            q, cot = other[:, :width].astype(BF16), other[:, width:].astype(BF16)
        pre = fold(nt(stack_ab, q))
        p, g = pre[:hidden_units], pre[hidden_units:]
        e = fold(nt(stack_c, cot))
        _, silu, slope = gate(g)
        hidden = silu * p
        pair = jnp.concatenate([e * silu, e * p * slope], axis=0)
        d_ab = fold(nn(two_terms(pair), q))
        hidden_two = two_terms(hidden)
        d_c = fold(nn(hidden_two, cot))
        lifted = jnp.concatenate([hidden_two, hidden_two[:hidden_units]], axis=0)
        out_ref[...] = tn(lifted, c_three).astype(out_ref.dtype)
        total = (d_ab, d_c) if total is None else (total[0] + d_ab, total[1] + d_c)
    for j, grad in enumerate(grads):
        grad[0] = total[0][j * units : (j + 1) * units]
        grad[1] = total[0][hidden_units + j * units : hidden_units + (j + 1) * units]
        grad[2] = total[1][j * units : (j + 1) * units]


def adjoint_kernel(stored, terms, units, parts, *refs):
    place_ref, first_ref, second_ref = refs[:3]
    adjoints = refs[3 : 3 + terms]
    stores = [(refs[3 + terms + 2 * i], refs[4 + terms + 2 * i]) for i in range(stored)]
    refs = refs[3 + terms + 2 * stored :]
    outs, (held, bases, blocks) = refs[:parts], refs[parts:]
    u_ab, u_c = flat(adjoints[0])
    for more in adjoints[1:]:
        ab, c = flat(more)
        u_ab, u_c = u_ab + ab, u_c + c
    held[0], held[1], held[2] = u_ab[:units], u_ab[units:], u_c
    bases[0], bases[1] = second_ref[...], first_ref[...]

    def step(i, carry):
        u_ab, u_c = flat(held)
        ab, c = flat(bases.at[i])
        stack_ab = two_terms(jnp.concatenate([ab, u_ab], axis=0))
        stack_c = two_terms(jnp.concatenate([c, u_c], axis=0))
        u_ab, u_c = sweep(curvature_terms, stack_ab, stack_c, units, stores, (u_ab, u_c))
        held[0], held[1], held[2] = u_ab[:units], u_ab[units:], u_c
        return carry

    lax.fori_loop(0, 2, step, 0)
    u_ab, u_c = flat(held)
    rows = jnp.concatenate([u_ab[:units], u_ab[units:], u_c], axis=1)
    share = rows.shape[1] // parts
    mine = place_ref[0]
    for target in range(parts):
        blocks[target] = rows[:, target * share : (target + 1) * share]
    for k, out_ref in enumerate(outs):
        out_ref[...] = blocks[lax.rem(mine + k, parts)]


def final_kernel(paired, units, *refs):
    place_ref = refs[0]
    parts = refs[1:-2]
    out_ref, held = refs[-2:]
    if paired:
        here = place_ref[0]
        for mask, part in enumerate(parts):
            source = here ^ mask
            place = (source & 1) * (PAIRED // 2) + (source >> 1)
            held[pl.ds(pl.multiple_of(place * units, units), units), :] = part[...]
    else:
        for j in range(parts[0].shape[0]):
            held[j * units : (j + 1) * units, :] = parts[0][j]
    out_ref[...] = held[...].T


def prepare_kernel(paired, divisor, *refs):
    place_ref, keys, values, rates, weights, first, second, column, held = refs
    half, width = keys.shape[0] // 2, keys.shape[1]
    units = column.shape[0]
    for at, message in ((0, first), (half, second)):
        message[:half, :width] = keys[at : at + half, :].astype(F32)
        message[:half, width:] = values[at : at + half, :].astype(F32)
        message[half:, :half] = jnp.broadcast_to(rates[:, at : at + half] / divisor, (PAD, half))
        message[half:, half:] = jnp.zeros((PAD, 2 * width - half), F32)
    held[...] = weights[...].T
    here = place_ref[0]
    group = (here & 1) * (PAIRED // 2) + (here >> 1) if paired else here
    column[...] = held[pl.ds(pl.multiple_of(group * units, units), units), :]


def size_of(x):
    return math.prod(x.shape) * x.dtype.itemsize


def call(kernel, out_shape, cost, inputs, smem=(), scratch=(), grant=0):
    specs = [
        pl.BlockSpec(memory_space=pltpu.SMEM if i in smem else pltpu.VMEM)
        for i in range(len(inputs))
    ]
    out_specs = jax.tree.map(lambda _: pl.BlockSpec(memory_space=pltpu.VMEM), out_shape)
    held = sum(size_of(x) for x in list(inputs) + jax.tree.leaves(out_shape))
    return pl.pallas_call(
        kernel,
        out_shape=out_shape,
        in_specs=specs,
        out_specs=out_specs,
        scratch_shapes=list(scratch),
        compiler_params=pltpu.CompilerParams(
            vmem_limit_bytes=max(min(60 * MIB, held + 12 * MIB), grant * MIB)
        ),
        cost_estimate=pl.CostEstimate(flops=cost, bytes_accessed=0, transcendentals=0),
    )(*inputs)


def body(queries, key_rows, value_rows, step_rates, cotangent, fast_init):
    tokens, width = queries.shape[1:]
    hidden = fast_init.shape[1]
    shards = lax.axis_size("seq")
    parts = lax.axis_size("batch")
    units = hidden // shards
    divisor = math.sqrt(shards * tokens)
    here = lax.axis_index("seq").astype(jnp.int32)[None]
    row = lax.axis_index("batch").astype(jnp.int32)[None]
    paired = shards == PAIRED
    half = tokens // 2
    share = 3 * width // parts
    block = jax.ShapeDtypeStruct((3, units, width), F32)
    column_block = jax.ShapeDtypeStruct((units, share), F32)

    def swap(x, mask):
        return lax.ppermute(x, "seq", [(i, i ^ mask) for i in range(shards)])

    def turn(x, k):
        return lax.ppermute(x, "batch", [(i, (i + k) % parts) for i in range(parts)])

    packed = jax.ShapeDtypeStruct((half + PAD, 2 * width), F32)
    *own, column = call(
        lambda *refs: prepare_kernel(paired, divisor, *refs),
        (packed, packed, column_block),
        1000,
        [here, key_rows[0], value_rows[0], step_rates, fast_init],
        smem=(0,),
        scratch=[pltpu.VMEM((hidden, share), F32)],
        grant=60,
    )

    def first(start, messages):
        count = len(messages)
        outs = (
            block,
            jax.ShapeDtypeStruct((count * half, 2 * width), BF16),
            jax.ShapeDtypeStruct((PAD, count * half), F32),
        )
        columns = 0 if len(start) == 2 else len(start) - 1
        return call(
            lambda *refs: first_kernel(count, columns, units, width, *refs),
            (block,) * (columns > 0) + outs,
            2 * 2 * 6 * count * half * width * units,
            start + messages,
            smem=(0,) if columns else (),
            scratch=[pltpu.VMEM((parts, units, share), F32)] if columns else (),
        )

    if paired:
        x = [None, None]
        y = [None, None]
        x[0], y[1] = swap(own[0], 2), swap(own[1], 4)
        columns = [column] + [turn(column, k) for k in range(1, parts)]
        x[1], y[0] = swap(own[1], 2), swap(own[0], 4)
        across = swap(x[0], 4)
        diagonal = [across, swap(y[1], 2)]
        near = own + [swap(m, 1) for m in own]
        initial, partial, *store_a = first([row] + columns, near)
        x[1], y[0], partial = lax.optimization_barrier((x[1], y[0], partial))
        side = x + y
        side = side + [swap(m, 1) for m in side]
        partial, *store_b = first([partial, initial], side)
        *diagonal, partial = lax.optimization_barrier((*diagonal, partial))
        far = diagonal + [swap(m, 1) for m in diagonal]
        middle, *store_c = first([partial, initial], far)
        stores = [*store_a, *store_b, *store_c]
    else:
        initial = lax.all_gather(column, "batch", axis=1, tiled=True)
        initial = jnp.stack(jnp.split(initial, 3, axis=1))
        every = lax.all_gather(jnp.stack(own), "seq", axis=0, tiled=True)
        kv = every[:, :half].astype(BF16).reshape(2 * shards * half, 2 * width)
        stores = [kv, every[:, half, :half].reshape(1, -1)]
        middle = None

    def ascend(base):
        return call(
            lambda *refs: second_kernel(len(stores) // 2, units, *refs),
            block,
            2 * 2 * 6 * shards * tokens * width * units,
            [base] + stores,
        )

    if middle is None:
        middle = ascend(initial)
    last = ascend(middle)

    cost = 2 * 2 * 7 * tokens * width * hidden
    if paired:
        pair = jnp.concatenate([queries[0].astype(F32), cotangent[0].astype(F32)], axis=1)
        other = swap(pair, 1)
        weights = [last, swap(last, 2), swap(last, 4), swap(last, 6)]
        part = jax.ShapeDtypeStruct((tokens, width), F32)
        kept, given, *grads = call(
            lambda *refs: outer_kernel(4, False, units, width, *refs),
            (part, part) + (block,) * 4,
            cost,
            weights + [queries[0], cotangent[0], other],
        )
        adjoints = [grads[0], swap(grads[1], 2), swap(grads[2], 4), swap(grads[3], 6)]
        result = (kept + swap(given, 1)).astype(BF16)
        result, adjoints[0] = lax.optimization_barrier((result, adjoints[0]))
    else:
        weights = lax.all_gather(last, "seq", axis=0, tiled=False)
        result, grads = call(
            lambda *refs: outer_kernel(shards, True, units, width, *refs),
            (
                jax.ShapeDtypeStruct((tokens, width), BF16),
                jax.ShapeDtypeStruct((shards, 3, units, width), F32),
            ),
            cost,
            [weights, queries[0], cotangent[0]],
        )
        adjoints = [lax.psum_scatter(grads, "seq", scatter_dimension=0, tiled=False)]

    rolled = call(
        lambda *refs: adjoint_kernel(len(stores) // 2, len(adjoints), units, parts, *refs),
        (column_block,) * parts,
        2 * 2 * 24 * shards * tokens * width * units,
        [row, initial, middle] + adjoints + stores,
        smem=(0,),
        scratch=[
            pltpu.VMEM((3, units, width), F32),
            pltpu.VMEM((2, 3, units, width), F32),
            pltpu.VMEM((parts, units, share), F32),
        ],
    )
    summed = rolled[0]
    for k in range(1, parts):
        summed = summed + turn(rolled[k], k)
    if paired:
        ring = [summed] + [swap(summed, mask) for mask in (2, 4, 6)]
        pieces = []
        for piece in ring:
            pieces += [piece, swap(piece, 1)]
    else:
        pieces = [lax.all_gather(summed, "seq", axis=0, tiled=False)]
    grad = call(
        lambda *refs: final_kernel(paired, units, *refs),
        jax.ShapeDtypeStruct((share, hidden), F32),
        1000,
        [here] + pieces,
        smem=(0,),
        scratch=[pltpu.VMEM((hidden, share), F32)],
    )
    return result[None], grad


def solution(mesh):
    placed = (
        P("batch", "seq", None),
        P("batch", "seq", None),
        P("batch", "seq", None),
        P("batch", "seq"),
        P("batch", "seq", None),
        P("batch", None),
    )

    return jax.shard_map(
        body,
        mesh=mesh,
        in_specs=placed,
        out_specs=(P("batch", "seq", None), P("batch", None)),
        check_vma=False,
    )
```

```python
import math

import jax
import jax.numpy as jnp
from jax import lax
from jax.experimental import pallas as pl
from jax.experimental.pallas import tpu as pltpu
from jax.sharding import PartitionSpec as P


F32 = jnp.float32
BF16 = jnp.bfloat16
PAIRED = 8
CHUNK = 1024
MIB = 1024 * 1024


def nt(left, right):
    return lax.dot_general(left, right, (((1,), (1,)), ((), ())), preferred_element_type=F32)


def nn(left, right):
    return lax.dot_general(left, right, (((1,), (0,)), ((), ())), preferred_element_type=F32)


def tn(left, right):
    return lax.dot_general(left, right, (((0,), (0,)), ((), ())), preferred_element_type=F32)


def two_terms(x):
    high = x.astype(BF16).astype(F32)
    return jnp.concatenate([x, x - high], axis=0).astype(BF16)


def fold(x):
    half = x.shape[0] // 2
    return x[:half] + x[half:]


def gate(g):
    decay = jnp.exp(-jnp.abs(g))
    sig = jnp.where(g >= 0, 1.0, decay) / (1.0 + decay)
    silu = g * sig
    slope = sig + silu * (1.0 - sig)
    return sig, silu, slope


def forward(stack_ab, stack_c, keys, values):
    return nt(stack_ab, keys), nt(stack_c, values)


def ascent_terms(units, pre, cross, keys, values, eta):
    pre = fold(pre)
    p, g = pre[:units], pre[units:]
    e = eta * fold(cross)
    _, silu, slope = gate(g)
    pair = jnp.concatenate([e * silu, e * p * slope], axis=0)
    hidden = eta * (silu * p)
    return fold(nn(two_terms(pair), keys)), fold(nn(two_terms(hidden), values))


def curvature_terms(units, pre, cross, keys, values, eta):
    pre = fold(pre)
    p, g = pre[:units], pre[units : 2 * units]
    tp, tg = pre[2 * units : 3 * units], pre[3 * units :]
    both = fold(cross)
    e, te = eta * both[:units], eta * both[units:]
    sig, silu, slope = gate(g)
    bend = sig * (1.0 - sig) * (2.0 + g * (1.0 - 2.0 * sig))
    slope_tg = slope * tg
    pair = jnp.concatenate(
        [te * silu + e * slope_tg, slope * (te * p + e * tp) + e * p * (bend * tg)], axis=0
    )
    hidden = eta * (slope_tg * p + silu * tp)
    return fold(nn(two_terms(pair), keys)), fold(nn(two_terms(hidden), values))


def flat(ref):
    return jnp.concatenate([ref[0], ref[1]], axis=0), ref[2]


def sweep(terms, stack_ab, stack_c, units, stores, acc):
    def load(kv, eta, start, size):
        width = kv.shape[1] // 2
        rows = pl.ds(start, size)
        return kv[rows, :width].astype(BF16), kv[rows, width:].astype(BF16), eta[0:1, rows]

    chunks = [
        (kv, eta, start, min(CHUNK, kv.shape[0] - start))
        for kv, eta in stores
        for start in range(0, kv.shape[0], CHUNK)
    ]
    if len(chunks) <= PAIRED:
        now = load(*chunks[0])
        pre = forward(stack_ab, stack_c, *now[:2])
        for i in range(len(chunks)):
            if i + 1 < len(chunks):
                later = load(*chunks[i + 1])
                ahead = forward(stack_ab, stack_c, *later[:2])
            ab, c = terms(units, *pre, *now)
            acc = acc[0] + ab, acc[1] + c
            if i + 1 < len(chunks):
                now, pre = later, ahead
        return acc
    for kv, eta in stores:

        def step(i, acc, kv=kv, eta=eta):
            now = load(kv, eta, pl.multiple_of(i * CHUNK, CHUNK), CHUNK)
            ab, c = terms(units, *forward(stack_ab, stack_c, *now[:2]), *now)
            return acc[0] + ab, acc[1] + c

        acc = lax.fori_loop(0, kv.shape[0] // CHUNK, step, acc)
    return acc


def first_kernel(messages, columns, units, width, *refs):
    if columns:
        place_ref, pieces, refs = refs[0], refs[1 : 1 + columns], refs[1 + columns :]
        base_ref, acc_ref, kv_ref, eta_ref, blocks = refs[-5:]
        mine = place_ref[0]
        for k, piece in enumerate(pieces):
            blocks[lax.rem(mine - k + columns, columns)] = piece[...]
        rows = jnp.concatenate([blocks[k] for k in range(columns)], axis=1)
        for j in range(3):
            base_ref[j] = rows[:, j * width : (j + 1) * width]
        start_ref = base_ref
    else:
        start_ref, base_ref = refs[0], refs[1]
        acc_ref, kv_ref, eta_ref = refs[-3:]
        refs = refs[2:]
    for i, part in enumerate(refs[:messages]):
        size = part.shape[0]
        kv_ref[i * size : (i + 1) * size, :] = part[...].astype(BF16)
    for i in range(messages // 2):
        rates = refs[messages + i]
        size = rates.shape[1]
        eta_ref[:, i * size : (i + 1) * size] = rates[...]
    ab, c = flat(base_ref)
    acc = sweep(
        ascent_terms, two_terms(ab), two_terms(c), units, [(kv_ref, eta_ref)], flat(start_ref)
    )
    acc_ref[0], acc_ref[1], acc_ref[2] = acc[0][:units], acc[0][units:], acc[1]


def second_kernel(stored, units, *refs):
    start_ref = refs[0]
    stores = [(refs[1 + 2 * i], refs[2 + 2 * i]) for i in range(stored)]
    out_ref = refs[1 + 2 * stored]
    ab, c = flat(start_ref)
    ab, c = sweep(ascent_terms, two_terms(ab), two_terms(c), units, stores, (ab, c))
    out_ref[0], out_ref[1], out_ref[2] = ab[:units], ab[units:], c


def outer_kernel(groups, stacked, units, width, *refs):
    weights = [refs[0].at[j] for j in range(groups)] if stacked else refs[:groups]
    refs = refs[1:] if stacked else refs[groups:]
    queries, cots = refs[0], refs[1]
    tokens = queries.shape[0]
    twin = len(refs) > 2 and refs[2].shape == (tokens, 2 * width) and refs[2].dtype == F32
    other = refs[2] if twin else None
    refs = refs[3:] if twin else refs[2:]
    outs = refs[:2] if twin else refs[:1]
    refs = refs[len(outs) :]
    grads = [refs[0].at[j] for j in range(groups)] if stacked else refs
    hidden_units = groups * units
    ab = jnp.concatenate([w[0] for w in weights] + [w[1] for w in weights], axis=0)
    c = jnp.concatenate([w[2] for w in weights], axis=0)
    stack_ab, stack_c = two_terms(ab), two_terms(c)
    c_high = stack_c[:hidden_units]
    c_three = jnp.concatenate([c_high, c_high, stack_c[hidden_units:]], axis=0)
    total = None
    for index, out_ref in enumerate(outs):
        if index == 0:
            q, cot = queries[...], cots[...]
        else:
            q, cot = other[:, :width].astype(BF16), other[:, width:].astype(BF16)
        pre = fold(nt(stack_ab, q))
        p, g = pre[:hidden_units], pre[hidden_units:]
        e = fold(nt(stack_c, cot))
        _, silu, slope = gate(g)
        hidden = silu * p
        pair = jnp.concatenate([e * silu, e * p * slope], axis=0)
        d_ab = fold(nn(two_terms(pair), q))
        hidden_two = two_terms(hidden)
        d_c = fold(nn(hidden_two, cot))
        lifted = jnp.concatenate([hidden_two, hidden_two[:hidden_units]], axis=0)
        out_ref[...] = tn(lifted, c_three).astype(out_ref.dtype)
        total = (d_ab, d_c) if total is None else (total[0] + d_ab, total[1] + d_c)
    for j, grad in enumerate(grads):
        grad[0] = total[0][j * units : (j + 1) * units]
        grad[1] = total[0][hidden_units + j * units : hidden_units + (j + 1) * units]
        grad[2] = total[1][j * units : (j + 1) * units]


def adjoint_kernel(stored, terms, units, parts, *refs):
    place_ref, first_ref, second_ref = refs[:3]
    adjoints = refs[3 : 3 + terms]
    stores = [(refs[3 + terms + 2 * i], refs[4 + terms + 2 * i]) for i in range(stored)]
    refs = refs[3 + terms + 2 * stored :]
    outs, (held, bases, blocks) = refs[:parts], refs[parts:]
    u_ab, u_c = flat(adjoints[0])
    for more in adjoints[1:]:
        ab, c = flat(more)
        u_ab, u_c = u_ab + ab, u_c + c
    held[0], held[1], held[2] = u_ab[:units], u_ab[units:], u_c
    bases[0], bases[1] = second_ref[...], first_ref[...]

    def step(i, carry):
        u_ab, u_c = flat(held)
        ab, c = flat(bases.at[i])
        stack_ab = two_terms(jnp.concatenate([ab, u_ab], axis=0))
        stack_c = two_terms(jnp.concatenate([c, u_c], axis=0))
        u_ab, u_c = sweep(curvature_terms, stack_ab, stack_c, units, stores, (u_ab, u_c))
        held[0], held[1], held[2] = u_ab[:units], u_ab[units:], u_c
        return carry

    lax.fori_loop(0, 2, step, 0)
    u_ab, u_c = flat(held)
    rows = jnp.concatenate([u_ab[:units], u_ab[units:], u_c], axis=1)
    share = rows.shape[1] // parts
    mine = place_ref[0]
    for target in range(parts):
        blocks[target] = rows[:, target * share : (target + 1) * share]
    for k, out_ref in enumerate(outs):
        out_ref[...] = blocks[lax.rem(mine + k, parts)]


def final_kernel(paired, units, *refs):
    place_ref = refs[0]
    parts = refs[1:-2]
    out_ref, held = refs[-2:]
    if paired:
        here = place_ref[0]
        for mask, part in enumerate(parts):
            source = here ^ mask
            place = (source & 1) * (PAIRED // 2) + (source >> 1)
            held[pl.ds(pl.multiple_of(place * units, units), units), :] = part[...]
    else:
        for j in range(parts[0].shape[0]):
            held[j * units : (j + 1) * units, :] = parts[0][j]
    out_ref[...] = held[...].T


def prepare_kernel(paired, divisor, *refs):
    place_ref, *sources = refs[:5]
    first, second, eta, column = refs[5:9]
    keys, values, rates, weights, held, sems = refs[9:]
    copies = [
        pltpu.make_async_copy(source, target, sems.at[i])
        for i, (source, target) in enumerate(zip(sources, (keys, values, rates, weights)))
    ]
    for copy in copies:
        copy.start()
    half, width = keys.shape[0] // 2, keys.shape[1]
    units = column.shape[0]
    copies[0].wait()
    first[:, :width] = keys[:half, :].astype(F32)
    second[:, :width] = keys[half:, :].astype(F32)
    copies[1].wait()
    first[:, width:] = values[:half, :].astype(F32)
    second[:, width:] = values[half:, :].astype(F32)
    copies[2].wait()
    eta[...] = rates[...] / divisor
    copies[3].wait()
    held[...] = weights[...].T
    here = place_ref[0]
    group = (here & 1) * (PAIRED // 2) + (here >> 1) if paired else here
    column[...] = held[pl.ds(pl.multiple_of(group * units, units), units), :]


def size_of(x):
    return math.prod(x.shape) * x.dtype.itemsize


def call(kernel, out_shape, cost, inputs, smem=(), scratch=(), far=(), grant=0):
    specs = [
        pl.BlockSpec(
            memory_space=pltpu.SMEM if i in smem else pltpu.HBM if i in far else pltpu.VMEM
        )
        for i in range(len(inputs))
    ]
    out_specs = jax.tree.map(lambda _: pl.BlockSpec(memory_space=pltpu.VMEM), out_shape)
    held = sum(size_of(x) for x in list(inputs) + jax.tree.leaves(out_shape))
    return pl.pallas_call(
        kernel,
        out_shape=out_shape,
        in_specs=specs,
        out_specs=out_specs,
        scratch_shapes=list(scratch),
        compiler_params=pltpu.CompilerParams(
            vmem_limit_bytes=max(min(60 * MIB, held + 12 * MIB), grant * MIB)
        ),
        cost_estimate=pl.CostEstimate(flops=cost, bytes_accessed=0, transcendentals=0),
    )(*inputs)


def body(queries, key_rows, value_rows, step_rates, cotangent, fast_init):
    tokens, width = queries.shape[1:]
    hidden = fast_init.shape[1]
    shards = lax.axis_size("seq")
    parts = lax.axis_size("batch")
    units = hidden // shards
    divisor = math.sqrt(shards * tokens)
    here = lax.axis_index("seq").astype(jnp.int32)[None]
    row = lax.axis_index("batch").astype(jnp.int32)[None]
    paired = shards == PAIRED
    half = tokens // 2
    share = 3 * width // parts
    block = jax.ShapeDtypeStruct((3, units, width), F32)
    column_block = jax.ShapeDtypeStruct((units, share), F32)

    def swap(x, mask):
        return lax.ppermute(x, "seq", [(i, i ^ mask) for i in range(shards)])

    def turn(x, k):
        return lax.ppermute(x, "batch", [(i, (i + k) % parts) for i in range(parts)])

    packed = jax.ShapeDtypeStruct((half, 2 * width), F32)
    *own, eta, column = call(
        lambda *refs: prepare_kernel(paired, divisor, *refs),
        (packed, packed, jax.ShapeDtypeStruct((1, tokens), F32), column_block),
        1000,
        [here, key_rows[0], value_rows[0], step_rates, fast_init],
        smem=(0,),
        far=(1, 2, 3, 4),
        grant=60,
        scratch=[
            pltpu.VMEM((tokens, width), BF16),
            pltpu.VMEM((tokens, width), BF16),
            pltpu.VMEM((1, tokens), F32),
            pltpu.VMEM((share, hidden), F32),
            pltpu.VMEM((hidden, share), F32),
            pltpu.SemaphoreType.DMA((4,)),
        ],
    )

    def first(start, messages, rates):
        count = len(messages)
        outs = (
            block,
            jax.ShapeDtypeStruct((count * half, 2 * width), BF16),
            jax.ShapeDtypeStruct((1, count * half), F32),
        )
        columns = 0 if len(start) == 2 else len(start) - 1
        return call(
            lambda *refs: first_kernel(count, columns, units, width, *refs),
            (block,) * (columns > 0) + outs,
            2 * 2 * 6 * count * half * width * units,
            start + messages + rates,
            smem=(0,) if columns else (),
            scratch=[pltpu.VMEM((parts, units, share), F32)] if columns else (),
        )

    if paired:
        x = [None, None]
        y = [None, None]
        x[0], y[1] = swap(own[0], 2), swap(own[1], 4)
        x[1], y[0] = swap(own[1], 2), swap(own[0], 4)
        columns = [column] + [turn(column, k) for k in range(1, parts)]
        rates = [eta] + [swap(eta, mask) for mask in range(1, PAIRED)]
        across = swap(x[0], 4)
        diagonal = [across, swap(y[1], 2)]
        near = own + [swap(m, 1) for m in own]
        initial, partial, *store_a = first([row] + columns, near, rates[0:2])
        x[1], y[0], partial = lax.optimization_barrier((x[1], y[0], partial))
        side = x + y
        side = side + [swap(m, 1) for m in side]
        order = [rates[mask] for mask in (2, 4, 3, 5)]
        partial, *store_b = first([partial, initial], side, order)
        *diagonal, partial = lax.optimization_barrier((*diagonal, partial))
        far = diagonal + [swap(m, 1) for m in diagonal]
        middle, *store_c = first([partial, initial], far, rates[6:8])
        stores = [*store_a, *store_b, *store_c]
    else:
        initial = lax.all_gather(column, "batch", axis=1, tiled=True)
        initial = jnp.stack(jnp.split(initial, 3, axis=1))
        every = lax.all_gather(jnp.stack(own), "seq", axis=0, tiled=True)
        every = every.reshape(2 * shards * half, 2 * width)
        stores = [every, lax.all_gather(eta, "seq", axis=1, tiled=True)]
        middle = None

    def ascend(base):
        return call(
            lambda *refs: second_kernel(len(stores) // 2, units, *refs),
            block,
            2 * 2 * 6 * shards * tokens * width * units,
            [base] + stores,
        )

    if middle is None:
        middle = ascend(initial)
    last = ascend(middle)

    cost = 2 * 2 * 7 * tokens * width * hidden
    if paired:
        pair = jnp.concatenate([queries[0].astype(F32), cotangent[0].astype(F32)], axis=1)
        other = swap(pair, 1)
        corner = swap(last, 6)
        weights = [last, swap(last, 2), swap(last, 4), corner]
        part = jax.ShapeDtypeStruct((tokens, width), F32)
        kept, given, *grads = call(
            lambda *refs: outer_kernel(4, False, units, width, *refs),
            (part, part) + (block,) * 4,
            cost,
            weights + [queries[0], cotangent[0], other],
        )
        corner = swap(grads[3], 6)
        adjoints = [grads[0], swap(grads[1], 2), swap(grads[2], 4), corner]
        result = (kept + swap(given, 1)).astype(BF16)
        result, adjoints[0] = lax.optimization_barrier((result, adjoints[0]))
    else:
        weights = lax.all_gather(last, "seq", axis=0, tiled=False)
        result, grads = call(
            lambda *refs: outer_kernel(shards, True, units, width, *refs),
            (
                jax.ShapeDtypeStruct((tokens, width), BF16),
                jax.ShapeDtypeStruct((shards, 3, units, width), F32),
            ),
            cost,
            [weights, queries[0], cotangent[0]],
        )
        adjoints = [lax.psum_scatter(grads, "seq", scatter_dimension=0, tiled=False)]

    rolled = call(
        lambda *refs: adjoint_kernel(len(stores) // 2, len(adjoints), units, parts, *refs),
        (column_block,) * parts,
        2 * 2 * 24 * shards * tokens * width * units,
        [row, initial, middle] + adjoints + stores,
        smem=(0,),
        scratch=[
            pltpu.VMEM((3, units, width), F32),
            pltpu.VMEM((2, 3, units, width), F32),
            pltpu.VMEM((parts, units, share), F32),
        ],
    )
    summed = rolled[0]
    for k in range(1, parts):
        summed = summed + turn(rolled[k], k)
    if paired:
        corner = swap(summed, 6)
        ring = [summed, swap(summed, 2), swap(summed, 4), corner]
        pieces = []
        for piece in ring:
            pieces += [piece, swap(piece, 1)]
    else:
        pieces = [lax.all_gather(summed, "seq", axis=0, tiled=False)]
    grad = call(
        lambda *refs: final_kernel(paired, units, *refs),
        jax.ShapeDtypeStruct((share, hidden), F32),
        1000,
        [here] + pieces,
        smem=(0,),
        scratch=[pltpu.VMEM((hidden, share), F32)],
    )
    return result[None], grad


def solution(mesh):
    placed = (
        P("batch", "seq", None),
        P("batch", "seq", None),
        P("batch", "seq", None),
        P("batch", "seq"),
        P("batch", "seq", None),
        P("batch", None),
    )

    return jax.shard_map(
        body,
        mesh=mesh,
        in_specs=placed,
        out_specs=(P("batch", "seq", None), P("batch", None)),
        check_vma=False,
    )
```

```python
import math

import jax
import jax.numpy as jnp
from jax import lax
from jax.experimental import pallas as pl
from jax.experimental.pallas import tpu as pltpu
from jax.sharding import PartitionSpec as P


F32 = jnp.float32
BF16 = jnp.bfloat16
PAIRED = 8
CHUNK = 1024
MIB = 1024 * 1024


def nt(left, right):
    return lax.dot_general(left, right, (((1,), (1,)), ((), ())), preferred_element_type=F32)


def nn(left, right):
    return lax.dot_general(left, right, (((1,), (0,)), ((), ())), preferred_element_type=F32)


def tn(left, right):
    return lax.dot_general(left, right, (((0,), (0,)), ((), ())), preferred_element_type=F32)


def two_terms(x):
    high = x.astype(BF16).astype(F32)
    return jnp.concatenate([x, x - high], axis=0).astype(BF16)


def fold(x):
    half = x.shape[0] // 2
    return x[:half] + x[half:]


def gate(g):
    sig = 0.5 * jnp.tanh(0.5 * g) + 0.5
    silu = g * sig
    slope = sig + silu * (1.0 - sig)
    return sig, silu, slope


def forward(stack_ab, stack_c, keys, values):
    return nt(stack_ab, keys), nt(stack_c, values)


def ascent_terms(units, pre, cross, keys, values, eta):
    pre = fold(pre)
    p, g = pre[:units], pre[units:]
    e = eta * fold(cross)
    _, silu, slope = gate(g)
    pair = jnp.concatenate([e * silu, e * p * slope], axis=0)
    hidden = eta * (silu * p)
    return fold(nn(two_terms(pair), keys)), fold(nn(two_terms(hidden), values))


def curvature_terms(units, pre, cross, keys, values, eta):
    pre = fold(pre)
    p, g = pre[:units], pre[units : 2 * units]
    tp, tg = pre[2 * units : 3 * units], pre[3 * units :]
    both = fold(cross)
    e, te = eta * both[:units], eta * both[units:]
    sig, silu, slope = gate(g)
    bend = sig * (1.0 - sig) * (2.0 + g * (1.0 - 2.0 * sig))
    slope_tg = slope * tg
    pair = jnp.concatenate(
        [te * silu + e * slope_tg, slope * (te * p + e * tp) + e * p * (bend * tg)], axis=0
    )
    hidden = eta * (slope_tg * p + silu * tp)
    return fold(nn(two_terms(pair), keys)), fold(nn(two_terms(hidden), values))


def flat(ref):
    return jnp.concatenate([ref[0], ref[1]], axis=0), ref[2]


def sweep(terms, stack_ab, stack_c, units, stores, acc):
    def load(kv, eta, start, size):
        width = kv.shape[1] // 2
        rows = pl.ds(start, size)
        return kv[rows, :width].astype(BF16), kv[rows, width:].astype(BF16), eta[0:1, rows]

    chunks = [
        (kv, eta, start, min(CHUNK, kv.shape[0] - start))
        for kv, eta in stores
        for start in range(0, kv.shape[0], CHUNK)
    ]
    if len(chunks) <= PAIRED:
        now = load(*chunks[0])
        pre = forward(stack_ab, stack_c, *now[:2])
        for i in range(len(chunks)):
            if i + 1 < len(chunks):
                later = load(*chunks[i + 1])
                ahead = forward(stack_ab, stack_c, *later[:2])
            ab, c = terms(units, *pre, *now)
            acc = acc[0] + ab, acc[1] + c
            if i + 1 < len(chunks):
                now, pre = later, ahead
        return acc
    for kv, eta in stores:

        def step(i, acc, kv=kv, eta=eta):
            now = load(kv, eta, pl.multiple_of(i * CHUNK, CHUNK), CHUNK)
            ab, c = terms(units, *forward(stack_ab, stack_c, *now[:2]), *now)
            return acc[0] + ab, acc[1] + c

        acc = lax.fori_loop(0, kv.shape[0] // CHUNK, step, acc)
    return acc


def first_kernel(messages, columns, units, width, *refs):
    if columns:
        place_ref, pieces, refs = refs[0], refs[1 : 1 + columns], refs[1 + columns :]
        base_ref, acc_ref, kv_ref, eta_ref, blocks = refs[-5:]
        mine = place_ref[0]
        for k, piece in enumerate(pieces):
            blocks[lax.rem(mine - k + columns, columns)] = piece[...]
        rows = jnp.concatenate([blocks[k] for k in range(columns)], axis=1)
        for j in range(3):
            base_ref[j] = rows[:, j * width : (j + 1) * width]
        start_ref = base_ref
    else:
        start_ref, base_ref = refs[0], refs[1]
        acc_ref, kv_ref, eta_ref = refs[-3:]
        refs = refs[2:]
    for i, part in enumerate(refs[:messages]):
        size = part.shape[0]
        kv_ref[i * size : (i + 1) * size, :] = part[...].astype(BF16)
    size = refs[messages].shape[1]
    for i in range(kv_ref.shape[0] // size):
        rates = refs[messages + i]
        eta_ref[:, i * size : (i + 1) * size] = rates[...]
    ab, c = flat(base_ref)
    acc = sweep(
        ascent_terms, two_terms(ab), two_terms(c), units, [(kv_ref, eta_ref)], flat(start_ref)
    )
    acc_ref[0], acc_ref[1], acc_ref[2] = acc[0][:units], acc[0][units:], acc[1]


def second_kernel(stored, units, *refs):
    start_ref = refs[0]
    stores = [(refs[1 + 2 * i], refs[2 + 2 * i]) for i in range(stored)]
    out_ref = refs[1 + 2 * stored]
    ab, c = flat(start_ref)
    ab, c = sweep(ascent_terms, two_terms(ab), two_terms(c), units, stores, (ab, c))
    out_ref[0], out_ref[1], out_ref[2] = ab[:units], ab[units:], c


def outer_kernel(groups, stacked, units, width, *refs):
    weights = [refs[0].at[j] for j in range(groups)] if stacked else refs[:groups]
    refs = refs[1:] if stacked else refs[groups:]
    queries, cots = refs[0], refs[1]
    tokens = queries.shape[0]
    twin = len(refs) > 2 and refs[2].shape == (tokens, 2 * width) and refs[2].dtype == F32
    other = refs[2] if twin else None
    refs = refs[3:] if twin else refs[2:]
    outs = refs[:2] if twin else refs[:1]
    refs = refs[len(outs) :]
    grads = [refs[0].at[j] for j in range(groups)] if stacked else refs
    hidden_units = groups * units
    ab = jnp.concatenate([w[0] for w in weights] + [w[1] for w in weights], axis=0)
    c = jnp.concatenate([w[2] for w in weights], axis=0)
    stack_ab, stack_c = two_terms(ab), two_terms(c)
    c_high = stack_c[:hidden_units]
    c_three = jnp.concatenate([c_high, c_high, stack_c[hidden_units:]], axis=0)
    total = None
    for index, out_ref in enumerate(outs):
        if index == 0:
            q, cot = queries[...], cots[...]
        else:
            q, cot = other[:, :width].astype(BF16), other[:, width:].astype(BF16)
        pre = fold(nt(stack_ab, q))
        p, g = pre[:hidden_units], pre[hidden_units:]
        e = fold(nt(stack_c, cot))
        _, silu, slope = gate(g)
        hidden = silu * p
        pair = jnp.concatenate([e * silu, e * p * slope], axis=0)
        d_ab = fold(nn(two_terms(pair), q))
        hidden_two = two_terms(hidden)
        d_c = fold(nn(hidden_two, cot))
        lifted = jnp.concatenate([hidden_two, hidden_two[:hidden_units]], axis=0)
        out_ref[...] = tn(lifted, c_three).astype(out_ref.dtype)
        total = (d_ab, d_c) if total is None else (total[0] + d_ab, total[1] + d_c)
    for j, grad in enumerate(grads):
        grad[0] = total[0][j * units : (j + 1) * units]
        grad[1] = total[0][hidden_units + j * units : hidden_units + (j + 1) * units]
        grad[2] = total[1][j * units : (j + 1) * units]


def adjoint_kernel(stored, terms, units, parts, *refs):
    place_ref, first_ref, second_ref = refs[:3]
    adjoints = refs[3 : 3 + terms]
    stores = [(refs[3 + terms + 2 * i], refs[4 + terms + 2 * i]) for i in range(stored)]
    refs = refs[3 + terms + 2 * stored :]
    outs, (held, bases, blocks) = refs[:parts], refs[parts:]
    u_ab, u_c = flat(adjoints[0])
    for more in adjoints[1:]:
        ab, c = flat(more)
        u_ab, u_c = u_ab + ab, u_c + c
    held[0], held[1], held[2] = u_ab[:units], u_ab[units:], u_c
    bases[0], bases[1] = second_ref[...], first_ref[...]

    def step(i, carry):
        u_ab, u_c = flat(held)
        ab, c = flat(bases.at[i])
        stack_ab = two_terms(jnp.concatenate([ab, u_ab], axis=0))
        stack_c = two_terms(jnp.concatenate([c, u_c], axis=0))
        u_ab, u_c = sweep(curvature_terms, stack_ab, stack_c, units, stores, (u_ab, u_c))
        held[0], held[1], held[2] = u_ab[:units], u_ab[units:], u_c
        return carry

    lax.fori_loop(0, 2, step, 0)
    u_ab, u_c = flat(held)
    rows = jnp.concatenate([u_ab[:units], u_ab[units:], u_c], axis=1)
    share = rows.shape[1] // parts
    mine = place_ref[0]
    for target in range(parts):
        blocks[target] = rows[:, target * share : (target + 1) * share]
    for k, out_ref in enumerate(outs):
        out_ref[...] = blocks[lax.rem(mine + k, parts)]


def final_kernel(paired, units, *refs):
    place_ref = refs[0]
    parts = refs[1:-2]
    out_ref, held = refs[-2:]
    if paired:
        here = place_ref[0]
        for mask, part in enumerate(parts):
            source = here ^ mask
            place = (source & 1) * (PAIRED // 2) + (source >> 1)
            held[pl.ds(pl.multiple_of(place * units, units), units), :] = part[...]
    else:
        for j in range(parts[0].shape[0]):
            held[j * units : (j + 1) * units, :] = parts[0][j]
    out_ref[...] = held[...].T


def prepare_kernel(paired, divisor, *refs):
    place_ref, *sources = refs[:5]
    first, second, eta, column = refs[5:9]
    keys, values, rates, weights, held, sems = refs[9:]
    copies = [
        pltpu.make_async_copy(source, target, sems.at[i])
        for i, (source, target) in enumerate(zip(sources, (keys, values, rates, weights)))
    ]
    for copy in copies:
        copy.start()
    half, width = keys.shape[0] // 2, keys.shape[1]
    units = column.shape[0]
    copies[0].wait()
    first[:, :width] = keys[:half, :].astype(F32)
    second[:, :width] = keys[half:, :].astype(F32)
    copies[1].wait()
    first[:, width:] = values[:half, :].astype(F32)
    second[:, width:] = values[half:, :].astype(F32)
    copies[2].wait()
    eta[...] = rates[...] / divisor
    copies[3].wait()
    held[...] = weights[...].T
    here = place_ref[0]
    group = (here & 1) * (PAIRED // 2) + (here >> 1) if paired else here
    column[...] = held[pl.ds(pl.multiple_of(group * units, units), units), :]


def size_of(x):
    return math.prod(x.shape) * x.dtype.itemsize


def call(kernel, out_shape, cost, inputs, smem=(), scratch=(), far=(), grant=0):
    specs = [
        pl.BlockSpec(
            memory_space=pltpu.SMEM if i in smem else pltpu.HBM if i in far else pltpu.VMEM
        )
        for i in range(len(inputs))
    ]
    out_specs = jax.tree.map(lambda _: pl.BlockSpec(memory_space=pltpu.VMEM), out_shape)
    held = sum(size_of(x) for x in list(inputs) + jax.tree.leaves(out_shape))
    return pl.pallas_call(
        kernel,
        out_shape=out_shape,
        in_specs=specs,
        out_specs=out_specs,
        scratch_shapes=list(scratch),
        compiler_params=pltpu.CompilerParams(
            vmem_limit_bytes=max(min(60 * MIB, held + 12 * MIB), grant * MIB)
        ),
        cost_estimate=pl.CostEstimate(flops=cost, bytes_accessed=0, transcendentals=0),
    )(*inputs)


def body(queries, key_rows, value_rows, step_rates, cotangent, fast_init):
    tokens, width = queries.shape[1:]
    hidden = fast_init.shape[1]
    shards = lax.axis_size("seq")
    parts = lax.axis_size("batch")
    units = hidden // shards
    divisor = math.sqrt(shards * tokens)
    here = lax.axis_index("seq").astype(jnp.int32)[None]
    row = lax.axis_index("batch").astype(jnp.int32)[None]
    paired = shards == PAIRED
    half = tokens // 2
    share = 3 * width // parts
    block = jax.ShapeDtypeStruct((3, units, width), F32)
    column_block = jax.ShapeDtypeStruct((units, share), F32)

    def swap(x, mask):
        return lax.ppermute(x, "seq", [(i, i ^ mask) for i in range(shards)])

    def turn(x, k):
        return lax.ppermute(x, "batch", [(i, (i + k) % parts) for i in range(parts)])

    packed = jax.ShapeDtypeStruct((half, 2 * width), F32)
    *own, eta, column = call(
        lambda *refs: prepare_kernel(paired, divisor, *refs),
        (packed, packed, jax.ShapeDtypeStruct((1, tokens), F32), column_block),
        1000,
        [here, key_rows[0], value_rows[0], step_rates, fast_init],
        smem=(0,),
        far=(1, 2, 3, 4),
        grant=60,
        scratch=[
            pltpu.VMEM((tokens, width), BF16),
            pltpu.VMEM((tokens, width), BF16),
            pltpu.VMEM((1, tokens), F32),
            pltpu.VMEM((share, hidden), F32),
            pltpu.VMEM((hidden, share), F32),
            pltpu.SemaphoreType.DMA((4,)),
        ],
    )

    def first(start, messages, rates):
        count = len(messages)
        size = sum(m.shape[0] for m in messages)
        outs = (
            block,
            jax.ShapeDtypeStruct((size, 2 * width), BF16),
            jax.ShapeDtypeStruct((1, size), F32),
        )
        columns = 0 if len(start) == 2 else len(start) - 1
        return call(
            lambda *refs: first_kernel(count, columns, units, width, *refs),
            (block,) * (columns > 0) + outs,
            2 * 2 * 6 * size * width * units,
            start + messages + rates,
            smem=(0,) if columns else (),
            scratch=[pltpu.VMEM((parts, units, share), F32)] if columns else (),
        )

    if paired:
        x = [None, None]
        y = [None, None]
        x[0], y[1] = swap(own[0], 2), swap(own[1], 4)
        x[1], y[0] = swap(own[1], 2), swap(own[0], 4)
        columns = [column] + [turn(column, k) for k in range(1, parts)]
        rates = [eta] + [swap(eta, mask) for mask in range(1, PAIRED)]
        quarter = half // 2
        diagonal = [swap(x[0][:quarter], 4), swap(y[1][:quarter], 2)]
        diagonal += [swap(x[0][quarter:], 4), swap(y[1][quarter:], 2)]
        near = own + [swap(m, 1) for m in own]
        initial, partial, *store_a = first([row] + columns, near, rates[0:2])
        x[1], y[0], partial = lax.optimization_barrier((x[1], y[0], partial))
        side = x + y
        side = side + [swap(m, 1) for m in side]
        order = [rates[mask] for mask in (2, 4, 3, 5)]
        partial, *store_b = first([partial, initial], side, order)

        def picked(rate, k):
            return jnp.concatenate(
                [rate[:, at + k * quarter : at + (k + 1) * quarter] for at in (0, half)], axis=1
            )

        early, late = diagonal[:2], diagonal[2:]
        *early, partial = lax.optimization_barrier((*early, partial))
        early += [swap(m, 1) for m in early]
        partial, *store_c = first(
            [partial, initial], early, [picked(rate, 0) for rate in rates[6:8]]
        )
        *late, partial = lax.optimization_barrier((*late, partial))
        late += [swap(m, 1) for m in late]
        middle, *store_d = first([partial, initial], late, [picked(rate, 1) for rate in rates[6:8]])
        stores = [*store_a, *store_b, *store_c, *store_d]
    else:
        initial = lax.all_gather(column, "batch", axis=1, tiled=True)
        initial = jnp.stack(jnp.split(initial, 3, axis=1))
        every = lax.all_gather(jnp.stack(own), "seq", axis=0, tiled=True)
        every = every.reshape(2 * shards * half, 2 * width)
        stores = [every, lax.all_gather(eta, "seq", axis=1, tiled=True)]
        middle = None

    def ascend(base):
        return call(
            lambda *refs: second_kernel(len(stores) // 2, units, *refs),
            block,
            2 * 2 * 6 * shards * tokens * width * units,
            [base] + stores,
        )

    if middle is None:
        middle = ascend(initial)
    last = ascend(middle)

    cost = 2 * 2 * 7 * tokens * width * hidden
    if paired:
        pair = jnp.concatenate([queries[0].astype(F32), cotangent[0].astype(F32)], axis=1)
        other = swap(pair, 1)
        corner = swap(last, 6)
        weights = [last, swap(last, 2), swap(last, 4), corner]
        part = jax.ShapeDtypeStruct((tokens, width), F32)
        kept, given, *grads = call(
            lambda *refs: outer_kernel(4, False, units, width, *refs),
            (part, part) + (block,) * 4,
            cost,
            weights + [queries[0], cotangent[0], other],
        )
        corner = swap(grads[3], 6)
        adjoints = [grads[0], swap(grads[1], 2), swap(grads[2], 4), corner]
        result = (kept + swap(given, 1)).astype(BF16)
        result, adjoints[0] = lax.optimization_barrier((result, adjoints[0]))
    else:
        weights = lax.all_gather(last, "seq", axis=0, tiled=False)
        result, grads = call(
            lambda *refs: outer_kernel(shards, True, units, width, *refs),
            (
                jax.ShapeDtypeStruct((tokens, width), BF16),
                jax.ShapeDtypeStruct((shards, 3, units, width), F32),
            ),
            cost,
            [weights, queries[0], cotangent[0]],
        )
        adjoints = [lax.psum_scatter(grads, "seq", scatter_dimension=0, tiled=False)]

    rolled = call(
        lambda *refs: adjoint_kernel(len(stores) // 2, len(adjoints), units, parts, *refs),
        (column_block,) * parts,
        2 * 2 * 24 * shards * tokens * width * units,
        [row, initial, middle] + adjoints + stores,
        smem=(0,),
        scratch=[
            pltpu.VMEM((3, units, width), F32),
            pltpu.VMEM((2, 3, units, width), F32),
            pltpu.VMEM((parts, units, share), F32),
        ],
    )
    summed = rolled[0]
    for k in range(1, parts):
        summed = summed + turn(rolled[k], k)
    if paired:
        corner = swap(summed, 6)
        ring = [summed, swap(summed, 2), swap(summed, 4), corner]
        pieces = []
        for piece in ring:
            pieces += [piece, swap(piece, 1)]
    else:
        pieces = [lax.all_gather(summed, "seq", axis=0, tiled=False)]
    grad = call(
        lambda *refs: final_kernel(paired, units, *refs),
        jax.ShapeDtypeStruct((share, hidden), F32),
        1000,
        [here] + pieces,
        smem=(0,),
        scratch=[pltpu.VMEM((hidden, share), F32)],
    )
    return result[None], grad


def solution(mesh):
    placed = (
        P("batch", "seq", None),
        P("batch", "seq", None),
        P("batch", "seq", None),
        P("batch", "seq"),
        P("batch", "seq", None),
        P("batch", None),
    )

    return jax.shard_map(
        body,
        mesh=mesh,
        in_specs=placed,
        out_specs=(P("batch", "seq", None), P("batch", None)),
        check_vma=False,
    )
```
